128 devices in a mesh: rep: 2 (over core), dp: 64 (over x, y, z).
Axes of the slice: x: 4, y: 4, z: 4, core: 2. Of those that a mesh axis runs over, the one named last changes fastest.
Arguments:
- x: bfloat16 [128, 1024, 1280], P(('rep', 'dp')), parts along dimension 0
- dy: bfloat16 [128, 1024, 1280], P(('rep', 'dp')), parts along dimension 0
- wq: bfloat16 [1, 1280, 3072], replicated
- wk: bfloat16 [1, 1280, 256], replicated
- wv: bfloat16 [1, 1280, 256], replicated
- wo: bfloat16 [1, 3072, 1280], replicated
- w_gate: bfloat16 [1, 1280, 3072], replicated
- w_up: bfloat16 [1, 1280, 3072], replicated
- w_down: bfloat16 [1, 3072, 1280], replicated
- m_wq: float32 [1, 1280, 3072], replicated
- m_wk: float32 [1, 1280, 256], replicated
- m_wv: float32 [1, 1280, 256], replicated
- m_wo: float32 [1, 3072, 1280], replicated
- m_w_gate: float32 [1, 1280, 3072], replicated
- m_w_up: float32 [1, 1280, 3072], replicated
- m_w_down: float32 [1, 3072, 1280], replicated
- v_wq: float32 [1, 1280, 3072], replicated
- v_wk: float32 [1, 1280, 256], replicated
- v_wv: float32 [1, 1280, 256], replicated
- v_wo: float32 [1, 3072, 1280], replicated
- v_w_gate: float32 [1, 1280, 3072], replicated
- v_w_up: float32 [1, 1280, 3072], replicated
- v_w_down: float32 [1, 3072, 1280], replicated
Outputs:
- output 1: bfloat16 [2, 1280, 3072], P('rep'), parts along dimension 0
- output 2: bfloat16 [2, 1280, 256], P('rep'), parts along dimension 0
- output 3: bfloat16 [2, 1280, 256], P('rep'), parts along dimension 0
- output 4: bfloat16 [2, 3072, 1280], P('rep'), parts along dimension 0
- output 5: bfloat16 [2, 1280, 3072], P('rep'), parts along dimension 0
- output 6: bfloat16 [2, 1280, 3072], P('rep'), parts along dimension 0
- output 7: bfloat16 [2, 3072, 1280], P('rep'), parts along dimension 0
- output 8: float32 [2, 1280, 3072], P('rep'), parts along dimension 0
- output 9: float32 [2, 1280, 256], P('rep'), parts along dimension 0
- output 10: float32 [2, 1280, 256], P('rep'), parts along dimension 0
- output 11: float32 [2, 3072, 1280], P('rep'), parts along dimension 0
- output 12: float32 [2, 1280, 3072], P('rep'), parts along dimension 0
- output 13: float32 [2, 1280, 3072], P('rep'), parts along dimension 0
- output 14: float32 [2, 3072, 1280], P('rep'), parts along dimension 0
- output 15: float32 [2, 1280, 3072], P('rep'), parts along dimension 0
- output 16: float32 [2, 1280, 256], P('rep'), parts along dimension 0
- output 17: float32 [2, 1280, 256], P('rep'), parts along dimension 0
- output 18: float32 [2, 3072, 1280], P('rep'), parts along dimension 0
- output 19: float32 [2, 1280, 3072], P('rep'), parts along dimension 0
- output 20: float32 [2, 1280, 3072], P('rep'), parts along dimension 0
- output 21: float32 [2, 3072, 1280], P('rep'), parts along dimension 0
There are 2 independent parts. The reference program is written for one: setup_inputs(seed, part) draws one part's arguments, and reference() takes and returns one part's arrays. A program takes and returns all parts, laid end to end along the dimension named above; an argument that names none is the same for every part.
All inputs are finite; a program needn't handle non-finite values.
Results may differ from the reference program's by a relative error of at most 0.024.
Values are sent between devices in bfloat16 or wider.
A program may use at most 1.5 GiB of HBM per device.

```python
import jax
import jax.numpy as jnp
from jax import lax

SEQUENCES = 64
TOKENS = 1024
D = 1280
HEADS = 24
KV_HEADS = 2
HEAD = 128
FF = 3072
LAYERS = 1
THETA = 10000
NAMES = ("wq", "wk", "wv", "wo", "w_gate", "w_up", "w_down")
SHAPES = {
    "wq": (LAYERS, D, HEADS * HEAD),
    "wk": (LAYERS, D, KV_HEADS * HEAD),
    "wv": (LAYERS, D, KV_HEADS * HEAD),
    "wo": (LAYERS, HEADS * HEAD, D),
    "w_gate": (LAYERS, D, FF),
    "w_up": (LAYERS, D, FF),
    "w_down": (LAYERS, FF, D),
}


def bump(key, n, height):
    away = (jnp.arange(n, dtype=jnp.int32) - jax.random.randint(key, (), 0, n, jnp.int32)) % n
    return jnp.where(away < n // 8, height, 1.0)


def together(key, own, strength):
    shared = jax.random.normal(key, own.shape[1:], jnp.float32)
    return (own + strength * shared) * lax.rsqrt(1 + strength * strength)


def setup_inputs(seed: int = 0, part: int = 0) -> dict:
    kx, kdy, ka, kb, kz, kf, kh, kl, *keys = jax.random.split(jax.random.key(seed), 8 + 3 * len(NAMES))
    kx, kdy, ka, kb = (jax.random.fold_in(k, part) for k in (kx, kdy, ka, kb))
    kw, km, kv = (keys[i::3] for i in range(3))
    shape = (SEQUENCES, TOKENS, D)
    much_x, much_dy = jax.random.uniform(kz, (2,), jnp.float32, 0.0, 1.0)
    loud = 2.0 ** jax.random.uniform(jax.random.fold_in(kz, 1), (), jnp.float32, -1.0, 2.0)
    layers = 2.0 ** jax.random.uniform(kl, (LAYERS, 1, 1), jnp.float32, -1.0, 1.0)
    times = {"wq": 1.0, "wk": 1.0, "wv": 2.0, "wo": layers, "w_gate": 1.0, "w_up": bump(kh, FF, 4.0), "w_down": layers}
    x = together(ka, jax.random.normal(kx, shape, jnp.float32), much_x) * bump(kf, D, 4.0)
    dy = together(kb, jax.random.normal(kdy, shape, jnp.float32), much_dy)
    drawn = {"x": x.astype(jnp.bfloat16), "dy": (loud * dy * (SEQUENCES * TOKENS) ** -0.5).astype(jnp.bfloat16)}
    for key, name in zip(kw, NAMES, strict=True):
        drawn[name] = (jax.random.normal(key, SHAPES[name], jnp.float32) * SHAPES[name][1] ** -0.5 * times[name]).astype(jnp.bfloat16)
    for key, name in zip(km, NAMES, strict=True):
        drawn[f"m_{name}"] = 0.1 * jax.random.normal(key, SHAPES[name], jnp.float32)
    for key, name in zip(kv, NAMES, strict=True):
        drawn[f"v_{name}"] = loud * loud * jax.random.uniform(key, SHAPES[name], jnp.float32, 0.2, 0.6)
    return drawn


def matmul(a, w):
    return jnp.dot(a, w, preferred_element_type=jnp.float32).astype(jnp.bfloat16)


def normed(h):
    wide = h.astype(jnp.float32)
    scale = lax.rsqrt(jnp.mean(wide**2, -1, keepdims=True) + 1e-6)
    return (wide * scale).astype(jnp.bfloat16)


def turned(t, theta):
    half = t.shape[-1] // 2
    angle = jnp.arange(t.shape[0], dtype=jnp.float32)[:, None] * theta ** (-jnp.arange(half, dtype=jnp.float32) / half)
    cos, sin = jnp.cos(angle)[:, None], jnp.sin(angle)[:, None]
    a, b = t[..., :half].astype(jnp.float32), t[..., half:].astype(jnp.float32)
    return jnp.concatenate([a * cos - b * sin, b * cos + a * sin], -1).astype(jnp.bfloat16)


def seen_by(q, k, v):
    tokens, kv = q.shape[0], k.shape[1]
    q = q.reshape(tokens, kv, -1, q.shape[-1])
    scores = jnp.einsum("tgsd,ugd->gstu", q.astype(jnp.float32), k.astype(jnp.float32)) * q.shape[-1] ** -0.5
    place = jnp.arange(tokens)
    weights = jax.nn.softmax(jnp.where(place[:, None] >= place, scores, -jnp.inf), -1).astype(jnp.bfloat16)
    return jnp.einsum("gstu,ugd->tgsd", weights.astype(jnp.float32), v.astype(jnp.float32)).astype(jnp.bfloat16).reshape(tokens, -1)


def layer(h, w):
    a = normed(h)
    q, k = (turned(matmul(a, w[name]).reshape(h.shape[0], -1, HEAD), THETA) for name in ("wq", "wk"))
    h = h + matmul(seen_by(q, k, matmul(a, w["wv"]).reshape(h.shape[0], -1, HEAD)), w["wo"])
    b = normed(h)
    gate = jnp.dot(b, w["w_gate"], preferred_element_type=jnp.float32)
    up = jnp.dot(b, w["w_up"], preferred_element_type=jnp.float32)
    return h + matmul((jax.nn.silu(gate) * up).astype(jnp.bfloat16), w["w_down"])


def adamw(w, m, v, g):
    m = 0.9 * m + 0.1 * g
    v = 0.95 * v + 0.05 * g * g
    step = m * lax.rsqrt(v + 1e-8) + 0.1 * w
    return (w - 0.02 * step).astype(jnp.bfloat16), m, v


def stack(weights, h):
    return lax.scan(lambda h, w: (layer(h, w), None), h, weights)[0]


def reference(x, dy, wq, wk, wv, wo, w_gate, w_up, w_down, m_wq, m_wk, m_wv, m_wo, m_w_gate, m_w_up, m_w_down, v_wq, v_wk, v_wv, v_wo, v_w_gate, v_w_up, v_w_down):
    weights = dict(zip(NAMES, (wq, wk, wv, wo, w_gate, w_up, w_down), strict=True))

    def take(so_far, sequence):
        h, by_y = sequence
        _, back = jax.vjp(stack, weights, h)
        by_weights, by_h = back(by_y)
        return jax.tree.map(lambda total, term: total + term.astype(jnp.float32), so_far, by_weights), by_h

    none_yet = {name: jnp.zeros(w.shape, jnp.float32) for name, w in weights.items()}
    by_weights, by_x = lax.scan(take, none_yet, (x, dy))
    gradients = [by_weights[name].astype(jnp.bfloat16).astype(jnp.float32) for name in NAMES]
    first = (m_wq, m_wk, m_wv, m_wo, m_w_gate, m_w_up, m_w_down)
    second = (v_wq, v_wk, v_wv, v_wo, v_w_gate, v_w_up, v_w_down)
    new = [adamw(weights[name].astype(jnp.float32), m, v, g) for name, m, v, g in zip(NAMES, first, second, gradients, strict=True)]
    return tuple(one[which] for which in range(3) for one in new)
```

```python
import functools
import math

import jax
import jax.numpy as jnp
import numpy as np
from jax import lax
from jax.experimental import pallas as pl
from jax.experimental.pallas import tpu as pltpu
from jax.sharding import PartitionSpec as P

BF, F32 = jnp.bfloat16, jnp.float32
T, D, F, HEADS, KV, HEAD = 1024, 1280, 3072, 24, 2, 128
GROUP = HEADS // KV
THETA = 10000
NAMES = ("wq", "wk", "wv", "wo", "w_gate", "w_up", "w_down")
NEG = -1e30
HIDDEN = 2 * NEG
LOG2E = 1.4426950408889634
SCALE = HEAD**-0.5
ANY = pl.BlockSpec(memory_space=pl.ANY)
MESH = pl.DeviceIdType.MESH
Q, L, HALF = 256, 128, 64
ROWS = range(0, T, Q)
ROOM = 63 * 2**20

CHUNKS, BLOCKS, COLOURS = 156, 26, 6
RB = 1024
LATE = 22


def loop(first, last, body):
    lax.fori_loop(first, last, lambda i, _: body(i), None)


def _dot(a, b, ca=1, cb=0):
    return lax.dot_general(a, b, (((ca,), (cb,)), ((), ())), preferred_element_type=F32)


def _rms(wide):
    return lax.rsqrt(jnp.mean(wide**2, -1, keepdims=True) + 1e-6)


def _angles():
    half = HALF
    angle = np.arange(T, dtype=np.float32)[:, None] * (np.float32(THETA) ** (-np.arange(half, dtype=np.float32) / half)).astype(np.float32)
    angle = angle.astype(np.float64)
    return np.concatenate([np.cos(angle), np.sin(angle)], 1).astype(np.float32)


def _qkv_kernel(x_ref, cs_ref, wq_ref, wk_ref, wv_ref, q_ref, k_ref, v_ref, at_ref, a_s, c_s, s_s):
    i = pl.program_id(0)

    def norm(r):
        wide = x_ref[r : r + Q, :].astype(F32)
        a_s[r : r + Q, :] = (wide * _rms(wide)).astype(BF)
        cs = cs_ref[r : r + Q, :]
        sc = pltpu.roll(cs, HALF, 1)
        low = lax.broadcasted_iota(jnp.int32, cs.shape, 1) < HALF
        c_s[r : r + Q, :] = jnp.where(low, cs, sc)
        s_s[r : r + Q, :] = jnp.where(low, -sc, cs)

    def heads(r, w_ref, out_ref, turn):
        got = _dot(a_s[r : r + Q, :], w_ref[...])
        for n in range(w_ref.shape[1] // HEAD):
            t = got[:, n * HEAD : (n + 1) * HEAD].astype(BF)
            if turn:
                t = t.astype(F32)
                t = (t * c_s[r : r + Q, :] + pltpu.roll(t, HALF, 1) * s_s[r : r + Q, :]).astype(BF)
            out_ref[n, r : r + Q, :] = t

    @pl.when(i == 0)
    def _():
        for r in ROWS:
            norm(r)
            heads(r, wq_ref, q_ref, True)

    @pl.when((i > 0) & (i < 6))
    def _():
        at_ref[...] = a_s[:, pl.ds(pl.multiple_of((i - 1) * Q, Q), Q)].T
        for r in ROWS:
            heads(r, wq_ref, q_ref, True)

    @pl.when(i == 6)
    def _():
        for r in ROWS:
            heads(r, wk_ref, k_ref, True)
            heads(r, wv_ref, v_ref, False)


def qkv(x, cs, wq, wk, wv):
    whole = lambda *shape: pl.BlockSpec(shape, lambda i: (0,) * len(shape))
    last = lambda i: jnp.minimum(i, 5)
    return pl.pallas_call(
        _qkv_kernel,
        grid=(7,),
        in_specs=[whole(T, D), whole(T, HEAD), pl.BlockSpec((D, 4 * HEAD), lambda i: (0, last(i))), whole(D, Q), whole(D, Q)],
        out_specs=[pl.BlockSpec((4, T, HEAD), lambda i: (last(i), 0, 0)), whole(KV, T, HEAD), whole(KV, T, HEAD),
                   pl.BlockSpec((Q, T), lambda i: (jnp.clip(i - 1, 0, 4), 0))],
        out_shape=[jax.ShapeDtypeStruct((HEADS, T, HEAD), BF), jax.ShapeDtypeStruct((KV, T, HEAD), BF),
                   jax.ShapeDtypeStruct((KV, T, HEAD), BF), jax.ShapeDtypeStruct((D, T), BF)],
        scratch_shapes=[pltpu.VMEM((T, D), BF), pltpu.VMEM((T, HEAD), F32), pltpu.VMEM((T, HEAD), F32)],
        compiler_params=pltpu.CompilerParams(vmem_limit_bytes=ROOM),
    )(x, cs, wq, wk, wv)


def _attend_kernel(q_ref, k_ref, v_ref, o_ref, ot_ref, lse_ref, top_s, mix_s, *, bq, bk, wide):
    iq = pl.program_id(1)
    cols = GROUP * bq
    e = SCALE * LOG2E
    pieces = range(0, cols, wide)
    top_s[...] = jnp.full((1, cols), NEG, F32)
    mix_s[...] = jnp.zeros((HEAD + 8, cols), F32)
    ones = jnp.ones((8, bk), BF)

    def block(j, masked):
        here = pl.ds(pl.multiple_of(j * bk, bk), bk)
        scores = [_dot(k_ref[0, here, :], q_ref[...].reshape(cols, HEAD)[at : at + wide, :], 1, 1) for at in pieces]
        values = jnp.concatenate([v_ref[0, here, :].T, ones], axis=0)
        if masked:
            gap = lax.rem(lax.broadcasted_iota(jnp.int32, (bk, wide), 1), bq) - lax.broadcasted_iota(jnp.int32, (bk, wide), 0)
            ok = gap >= j * bk - iq * bq
        weights, keeps = [], []
        for at, s in zip(pieces, scores):
            if masked:
                s = jnp.where(ok, s, HIDDEN)
            old = top_s[:, at : at + wide]
            top = jnp.maximum(old, s.max(axis=0, keepdims=True))
            top_s[:, at : at + wide] = top
            weights.append(jnp.exp2((s - top) * e).astype(BF))
            keeps.append(jnp.exp2((old - top) * e))
        for at, p, keep in zip(pieces, weights, keeps):
            mix_s[:, at : at + wide] = mix_s[:, at : at + wide] * keep + _dot(values, p)

    loop(0, lax.div(iq * bq, bk), lambda j: block(j, False))
    loop(lax.div(iq * bq, bk), lax.div(iq * bq + bq + bk - 1, bk), lambda j: block(j, True))
    top, total = top_s[...], mix_s[HEAD : HEAD + 1, :]
    inverse = 1 / total
    lse = top * SCALE + jnp.log(total)
    for n in range(GROUP):
        out = (mix_s[:HEAD, n * bq : (n + 1) * bq] * inverse[:, n * bq : (n + 1) * bq]).astype(BF)
        ot_ref[n * HEAD : (n + 1) * HEAD, :] = out
        o_ref[:, n * HEAD : (n + 1) * HEAD] = out.T
        lse_ref[n] = lse[:, n * bq : (n + 1) * bq]


def attend(q, k, v, bq=Q, bk=Q, wide=2 * Q):
    return pl.pallas_call(
        functools.partial(_attend_kernel, bq=bq, bk=bk, wide=wide),
        grid=(KV, T // bq),
        in_specs=[pl.BlockSpec((GROUP, bq, HEAD), lambda h, i: (h, i, 0)), pl.BlockSpec((1, T, HEAD), lambda h, i: (h, 0, 0)),
                  pl.BlockSpec((1, T, HEAD), lambda h, i: (h, 0, 0))],
        out_specs=[pl.BlockSpec((bq, GROUP * HEAD), lambda h, i: (i, h)), pl.BlockSpec((GROUP * HEAD, bq), lambda h, i: (h, i)),
                   pl.BlockSpec((GROUP, 1, bq), lambda h, i: (h, 0, i))],
        out_shape=[jax.ShapeDtypeStruct((T, HEADS * HEAD), BF), jax.ShapeDtypeStruct((HEADS * HEAD, T), BF),
                   jax.ShapeDtypeStruct((HEADS, 1, T), F32)],
        scratch_shapes=[pltpu.VMEM((1, GROUP * bq), F32), pltpu.VMEM((HEAD + 8, GROUP * bq), F32)],
        compiler_params=pltpu.CompilerParams(vmem_limit_bytes=ROOM),
            )(q, k, v)


def _out_kernel(o_ref, wo_ref, x_ref, h_ref, b_ref, bt_ref):
    h = (x_ref[...].astype(F32) + _dot(o_ref[...], wo_ref[...]).astype(BF).astype(F32)).astype(BF)
    h_ref[...] = h
    wide = h.astype(F32)
    b = (wide * _rms(wide)).astype(BF)
    b_ref[...] = b
    bt_ref[...] = b.T


def out_norm(o, wo, x, rows=Q):
    spec = lambda width: pl.BlockSpec((rows, width), lambda i: (i, 0))
    return pl.pallas_call(
        _out_kernel,
        grid=(T // rows,),
        in_specs=[spec(HEADS * HEAD), pl.BlockSpec((HEADS * HEAD, D), lambda i: (0, 0)), spec(D)],
        out_specs=[spec(D), spec(D), pl.BlockSpec((D, rows), lambda i: (0, i))],
        out_shape=[jax.ShapeDtypeStruct((T, D), BF), jax.ShapeDtypeStruct((T, D), BF), jax.ShapeDtypeStruct((D, T), BF)],
        compiler_params=pltpu.CompilerParams(vmem_limit_bytes=ROOM),
        cost_estimate=pl.CostEstimate(flops=2 * T * D * 3072, transcendentals=0, bytes_accessed=10**7),
    )(o, wo, x)


STRIDES = (16, 4, 1)


def near_bit(place):
    return (place + 1) // 2 % 2


def rows(at, n):
    return pl.ds(pl.multiple_of(at, 16), n)


def block_at(place):
    return (place >= 0) & (place < BLOCKS + 1) & (place != LATE), place - (place + 31 - LATE) // 32


class Comm:
    STEPS, SLOTS = 11, 4
    END = BLOCKS + 1 + 2 * STEPS

    @staticmethod
    def scratch():
        V, S, n = pltpu.VMEM, pltpu.SemaphoreType.DMA, Comm.SLOTS
        return [V((COLOURS, n, RB, L), BF), V((COLOURS, n, RB // 2, L), BF), V((COLOURS, 2, RB // 2, L), F32), V((COLOURS, n, RB // 2, L), BF),
                S((Comm.STEPS, COLOURS, n)), S((Comm.STEPS, COLOURS, n)), S((COLOURS, n)), S((COLOURS, n))]

    def __init__(self, g, r, refs):
        self.g, self.r = g, r
        self.recv, self.send, self.acc, self.loc, self.ssem, self.rsem, self.lsem, self.osem = refs
        dp = lax.axis_index("dp")
        place = [dp // n % 4 for n in STRIDES]
        self.bits = [[near_bit(c) for c in place], [c // 2 for c in place]]
        self.nexts = [[dp + (1 - c % 2 * 2) * n for c, n in zip(place, STRIDES)], [dp + (3 - 2 * c) * n for c, n in zip(place, STRIDES)]]

    def barrier(self):
        sem = pltpu.get_barrier_semaphore()
        for n in (*self.nexts[0], *self.nexts[1]):
            pl.semaphore_signal(sem, device_id={"dp": n}, device_id_type=MESH)
        pl.semaphore_wait(sem, COLOURS)

    def bit(self, c, k):
        return self.bits[(k ^ c) % 2][(c // 2 + k // 2) % 3]

    def partner(self, c, k):
        return self.nexts[(k ^ c) % 2][(c // 2 + k // 2) % 3]

    def row(self, c, k):
        at = 0
        for i in range(1, k):
            at = at + self.bit(c, i) * (RB >> (i + 1))
        return at

    def half(self, c, b, bit):
        return self.g.at[COLOURS * b + c, rows(bit * (RB // 2), RB // 2), :]

    def mine(self, c, b, k):
        return self.r[c].at[b, rows(self.row(c, k), RB >> k), :]

    def copy(self, s, c, b, p):
        k = s if s < 6 else self.STEPS - s
        n = RB >> (k + 1)
        if s < 6:
            src = self.half(c, b, 1 - self.bit(c, 0)) if s == 0 else self.send.at[c, p, pl.ds(RB // 2 - 2 * n, n), :]
            dst = self.recv.at[c, p, pl.ds(RB - 2 * n, n), :]
        else:
            dst = self.mine(c, b, k + 1)
            src = self.send.at[c, p, pl.ds(RB // 2 - n, n), :] if s == 6 else dst
        return pltpu.make_async_remote_copy(src_ref=src, dst_ref=dst, send_sem=self.ssem.at[s, c, p], recv_sem=self.rsem.at[s, c, p],
                                            device_id={"dp": self.partner(c, k)}, device_id_type=MESH)

    def local(self, c, b, p):
        return pltpu.make_async_copy(self.half(c, b, self.bit(c, 0)), self.loc.at[c, p], self.lsem.at[c, p])

    def own(self, c, b, p):
        n = RB >> 6
        return pltpu.make_async_copy(self.send.at[c, p, pl.ds(RB // 2 - n, n), :], self.mine(c, b, 6), self.osem.at[c, p])

    def step(self, s, b):
        p, pa = b % self.SLOTS, b % 2
        for c in range(COLOURS):
            if s:
                self.copy(s - 1, c, b, p).wait_recv()
            if s == 0:
                self.local(c, b, p).start()
            elif s <= 6:
                n = RB >> s
                h = n // 2 if s < 6 else n
                if s == 1:
                    self.local(c, b, p).wait()

                def total(at):
                    came = self.recv[c, p, rows(RB - 2 * n + at, h), :].astype(F32)
                    if s == 1:
                        return self.loc[c, p, rows(at, h), :].astype(F32) + came
                    return self.acc[c, pa, rows(RB // 2 - 2 * n + at, h), :] + came

                if s < 6:
                    self.send[c, p, RB // 2 - n : RB // 2 - n + h, :] = total((1 - self.bit(c, s)) * h).astype(BF)
                else:
                    self.send[c, p, RB // 2 - n :, :] = total(0).astype(BF)
                    self.own(c, b, p).start()
            elif s == 7:
                self.own(c, b, p).wait()
            if s < self.STEPS:
                self.copy(s, c, b, p).start()
            if 0 < s < 6:
                self.acc[c, pa, RB // 2 - n : RB // 2 - n + h, :] = total(self.bit(c, s) * h)

    def tick(self, t):
        for s in range(self.STEPS, -1, -1):
            valid, b = block_at(t - 2 * s)

            @pl.when(valid)
            def _():
                self.step(s, b)

            if s < self.STEPS:
                valid1, b1 = block_at(t - 2 * s - 2)

                @pl.when(valid1)
                def _():
                    for c in range(COLOURS):
                        self.copy(s, c, b1, b1 % self.SLOTS).wait_send()

    def ticks(self, first, last):
        loop(first, last, self.tick)


def _put(stage, value, k):
    stage[k, :Q, :] = value[:, :L].astype(BF)
    stage[k, Q:, :] = value[:, L:].astype(BF)


def _backward_kernel(b_ref, bt_ref, dy_ref, h_ref, wg_ref, wu_ref, wd_ref, ot_ref, wo_ref, q_ref, k_ref, v_ref, lse_ref, at_ref, cs_ref,
                     g_ref, *rest):
    r_refs, rest = rest[:6], rest[6:]
    stage, dh_s, dot_s, delta_s, isem, wsem, osem, *refs = rest
    comm = Comm(g_ref, r_refs, refs)
    comm.barrier()
    ticks = comm.ticks

    def load(src, dst, n):
        return pltpu.make_async_copy(src, dst, isem.at[n])

    def out(slot, unit, half):
        return pltpu.make_async_copy(stage.at[slot], g_ref.at[pl.ds(unit * 5, 5), pl.ds(half * 512, 512), :], osem.at[slot])

    def mlp(b_s, bt_s, dy_s, db_s, wg_s, wu_s, wd_s, act_s, dg_s, du_s):
        firsts = [load(b_ref, b_s, 0), load(bt_ref, bt_s, 1), load(dy_ref, dy_s, 2)]
        for d in firsts:
            d.start()

        def weights(j, slot):
            here = pl.ds(pl.multiple_of(j * Q, Q), Q)
            return [pltpu.make_async_copy(src, dst.at[slot], wsem.at[slot, n]) for n, (src, dst) in enumerate(
                ((wg_ref.at[:, here], wg_s), (wu_ref.at[:, here], wu_s), (wd_ref.at[here, :], wd_s)))]

        for d in weights(0, 0):
            d.start()
        db_s[...] = jnp.zeros_like(db_s)
        for d in firsts:
            d.wait()

        def outs(j):
            return [out(n, 3 * (j // 2) + n, j % 2) for n in range(3)]

        def upto_j(j):
            return jnp.maximum(j - 1, 0)

        def body(j):
            slot = j % 2

            @pl.when(j < 11)
            def _():
                for d in weights(j + 1, 1 - slot):
                    d.start()

            for d in weights(j, slot):
                d.wait()
            for r in ROWS:
                gate = _dot(b_s[r : r + Q, :], wg_s[slot])
                up = _dot(b_s[r : r + Q, :], wu_s[slot])
                da = _dot(dy_s[r : r + Q, :], wd_s[slot], 1, 1).astype(BF).astype(F32)
                sig = 1 / (1 + jnp.exp(-gate))
                silu = gate * sig
                act_s[:, r : r + Q] = (silu * up).astype(BF).T
                du_s[r : r + Q, :] = (da * silu).astype(BF)
                dg_s[r : r + Q, :] = (da * up * (sig + silu * (1 - sig))).astype(BF)

            @pl.when(j > 0)
            def _():
                for d in outs(j - 1):
                    d.wait()

            ticks(upto_j(j - 1), upto_j(j))
            for k in range(5):
                _put(stage.at[0], _dot(act_s[...], dy_s[:, k * Q : (k + 1) * Q]), k)
                _put(stage.at[1], _dot(bt_s[k * Q : (k + 1) * Q, :], dg_s[...]), k)
                _put(stage.at[2], _dot(bt_s[k * Q : (k + 1) * Q, :], du_s[...]), k)
            for d in outs(j):
                d.start()
            for r in ROWS:
                db_s[r : r + Q, :] += _dot(dg_s[r : r + Q, :], wg_s[slot], 1, 1) + _dot(du_s[r : r + Q, :], wu_s[slot], 1, 1)

        loop(0, 12, body)
        for d in outs(11):
            d.wait()
        load(h_ref, b_s, 0).start()
        load(h_ref, b_s, 0).wait()
        for r in range(0, T, L):
            wide = b_s[r : r + L, :].astype(F32)
            scale = _rms(wide)
            db = db_s[r : r + L, :].astype(BF).astype(F32)
            back = db * scale - wide * (scale**3 * jnp.mean(db * wide, -1, keepdims=True))
            dh_s[r : r + L, :] = (dy_s[r : r + L, :].astype(F32) + back.astype(BF).astype(F32)).astype(BF)

    V = pltpu.VMEM
    pl.run_scoped(mlp, V((T, D), BF), V((D, T), BF), V((T, D), BF), V((T, D), F32), V((2, D, Q), BF), V((2, D, Q), BF), V((2, Q, D), BF),
                  V((Q, T), BF), V((T, Q), BF), V((T, Q), BF))

    def rest_of_layer(ot_s, wo_s, q_s, dq_s, at_s, k_s, kt_s, v_s, lse_s, cs_s, cst_s, dqt_s, dk_s, dv_s):
        firsts = [load(s, d, n) for n, (s, d) in enumerate(
            ((q_ref, q_s), (at_ref, at_s), (k_ref, k_s), (v_ref, v_s), (lse_ref, lse_s), (cs_ref, cs_s)))]

        def parts(i, slot):
            here = pl.ds(pl.multiple_of(i * Q, Q), Q)
            return [pltpu.make_async_copy(ot_ref.at[here, :], ot_s.at[slot], wsem.at[slot, 0]),
                    pltpu.make_async_copy(wo_ref.at[here, :], wo_s.at[slot], wsem.at[slot, 1])]

        for d in parts(0, 0) + firsts:
            d.start()

        def outs(i):
            return out(i % 2, 18 + (i // 2), i % 2)

        def project(i):
            slot = i % 2

            @pl.when(i < 11)
            def _():
                for d in parts(i + 1, 1 - slot):
                    d.start()

            for d in parts(i, slot):
                d.wait()
            here = pl.ds(pl.multiple_of(i * Q, Q), Q)
            do = _dot(wo_s[slot], dh_s[...], 1, 1).astype(BF)
            dot_s[here, :] = do
            both = do.astype(F32) * ot_s[slot].astype(F32)
            for n in range(2):
                delta_s[2 * i + n] = both[n * L : (n + 1) * L, :].sum(0, keepdims=True)
            for k in range(5):
                _put(stage.at[slot], _dot(ot_s[slot], dh_s[:, k * Q : (k + 1) * Q]), k)
            outs(i).start()

            @pl.when(i > 0)
            def _():
                outs(i - 1).wait()

        e = SCALE * LOG2E
        bq, bk, wide = L, Q, 512
        cols = GROUP * bq

        def turned_back(t, here):
            t = t.astype(BF).astype(F32)
            cos, sin = cst_s[:HALF, here], cst_s[HALF:, here]
            a, b = t[:HALF, :], t[HALF:, :]
            return jnp.concatenate([a * cos + b * sin, b * cos - a * sin], 0).astype(BF)

        def attention(n):
            ih, iq = (n // 8), n % 8
            at = pl.ds(pl.multiple_of(iq * bq, bq), bq)
            heads = ih * GROUP

            @pl.when(iq == 0)
            def _():
                dk_s[...] = jnp.zeros_like(dk_s)
                dv_s[...] = jnp.zeros_like(dv_s)

            dqt_s[...] = jnp.zeros_like(dqt_s)

            def row(ref):
                return jnp.concatenate([ref[heads + m, :, at] for m in range(GROUP)], axis=1)

            lses, deltas = row(lse_s) * LOG2E, row(delta_s)

            def block(j, masked):
                here = pl.ds(pl.multiple_of(j * bk, bk), bk)
                kj, vj, ktj = k_s[ih, here, :], v_s[ih, here, :], kt_s[ih, :, here]
                if masked:
                    gap = lax.rem(lax.broadcasted_iota(jnp.int32, (bk, wide), 1), bq) - lax.broadcasted_iota(jnp.int32, (bk, wide), 0)
                    ok = gap >= j * bk - iq * bq
                per = wide // bq
                qs = [q_s[pl.ds(heads + m, per), at, :].reshape(wide, HEAD) for m in range(0, GROUP, per)]
                dos = [jnp.concatenate([dot_s[pl.ds(pl.multiple_of((heads + m + i) * HEAD, HEAD), HEAD), at] for i in range(per)], axis=1)
                       for m in range(0, GROUP, per)]
                scores = [_dot(kj, x, 1, 1) for x in qs]
                dps = [_dot(vj, x) for x in dos]
                for m in range(cols // wide):
                    span = slice(m * wide, (m + 1) * wide)
                    p = jnp.exp2(scores[m] * e - lses[:, span])
                    if masked:
                        p = jnp.where(ok, p, 0.0)
                    ds = (p * (dps[m] - deltas[:, span])).astype(BF)
                    dv_s[here, :] += _dot(p.astype(BF), dos[m], 1, 1)
                    dk_s[here, :] += _dot(ds, qs[m])
                    dqt_s[:, span] += _dot(ktj, ds)

            loop(0, iq // 2, lambda j: block(j, False))
            block(iq // 2, True)
            for m in range(GROUP):
                dq_s[m * HEAD : (m + 1) * HEAD, at] = turned_back(dqt_s[:, m * bq : (m + 1) * bq] * SCALE, at)

            @pl.when(iq == 7)
            def _():
                def product(i, part):
                    slot = i % 2

                    @pl.when(i > 1)
                    def _():
                        out(slot, 0, 0).wait()

                    for k in range(5):
                        _put(stage.at[slot], _dot(at_s[k * Q : (k + 1) * Q, :], part, 1, 1), k)

                def one(i):
                    product(i, dq_s[pl.ds(pl.multiple_of(i * Q, Q), Q), :])
                    out(i % 2, 24 + 3 * ih + (i // 2), i % 2).start()

                loop(0, 6, one)
                dk = turned_back((dk_s[...] * SCALE).T, pl.ds(0, T))
                product(6, jnp.concatenate([dk, dv_s[...].T.astype(BF)], 0))
                out(0, 30, ih).start()
                out(1, 0, 0).wait()
                out(0, 0, 0).wait()

        def done(n):
            return jnp.where(n < 12, 10 + (n + 1) // 3, jnp.where(n < 28, 14 + (n - 11) * 5 // 8, Comm.END))

        def body(n):
            @pl.when(n < 12)
            def _():
                project(n)

            @pl.when(n == 12)
            def _():
                outs(11).wait()
                for d in firsts:
                    d.wait()
                for i in range(KV):
                    kt_s[i] = k_s[i].T
                cst_s[...] = cs_s[...].T

            @pl.when((n >= 12) & (n < 28))
            def _():
                attention(n - 12)

            ticks(done(n - 1), done(n))

        loop(0, 29, body)

    pl.run_scoped(rest_of_layer, V((2, Q, T), BF), V((2, Q, D), BF), V((HEADS, T, HEAD), BF), V((GROUP * HEAD, T), BF), V((D, T), BF),
                  V((KV, T, HEAD), BF), V((KV, HEAD, T), BF), V((KV, T, HEAD), BF), V((HEADS, 1, T), F32), V((T, HEAD), F32), V((HEAD, T), F32),
                  V((HEAD, GROUP * L), F32), V((T, HEAD), F32), V((T, HEAD), F32))


def backward(b, bt, dy, h, wg, wu, wd, ot, wo, q, k, v, lse, at, cs):
    V, S = pltpu.VMEM, pltpu.SemaphoreType.DMA
    outs = pl.pallas_call(
        _backward_kernel,
        in_specs=[ANY] * 15,
        out_specs=[ANY] * 7,
        out_shape=[jax.ShapeDtypeStruct((CHUNKS, RB, L), BF)] + [jax.ShapeDtypeStruct((BLOCKS, RB // 2, L), BF)] * 6,
        scratch_shapes=[V((3, 5, 512, L), BF), V((T, D), BF), V((HEADS * HEAD, T), BF), V((HEADS, 1, T), F32), S((6,)), S((2, 3)), S((3,)),
                        *Comm.scratch()],
        compiler_params=pltpu.CompilerParams(collective_id=0, has_side_effects=True, vmem_limit_bytes=ROOM),
    )(b, bt, dy, h, wg, wu, wd, ot, wo, q, k, v, lse, at, cs)
    return outs[0], outs[1:]


def _adam_kernel(*refs, mine, depth):
    r_refs, old, new = refs[:6], refs[6:27], refs[-31:-10]
    g_s, w_s, m_s, v_s, wo_s, mo_s, vo_s, gsem, isem, osem = refs[-10:]
    dp = lax.axis_index("dp")
    ins, outs = (w_s, m_s, v_s), (wo_s, mo_s, vo_s)
    number = {name: i for i, name in enumerate(NAMES)}
    steps = CHUNKS // 2

    def chunk(i, u):
        axis = i % 3
        place = jnp.where(axis == 0, dp // STRIDES[0], jnp.where(axis == 1, dp // STRIDES[1] % 4, dp % 4))
        bit = place // 2 if u else near_bit(place)
        at = 2 * i + u
        return i // 3, axis, at // 5, at % 5, bit if mine else 1 - bit

    def places(unit, k, half):
        tall = lambda name, n: [(number[name], 512 * n + Q * half, Q * k + L * t) for t in range(2)]
        flat = lambda name, n: [(number[name], Q * k, 512 * n + Q * half + L * t) for t in range(2)]
        third = unit % 3
        return [((unit < 18) & (third == 0), tall("w_down", unit // 3)), ((unit < 18) & (third == 1), flat("w_gate", unit // 3)),
                ((unit < 18) & (third == 2), flat("w_up", unit // 3)), ((unit >= 18) & (unit < 24), tall("wo", unit - 18)),
                ((unit >= 24) & (unit < 30), flat("wq", unit - 24)),
                (unit == 30, [(number[name], Q * k, L * half) for name in ("wk", "wv")])]

    def tile(ref, row, col):
        return ref.at[pl.ds(pl.multiple_of(row, Q), Q), pl.ds(pl.multiple_of(col, L), L)]

    def moves(i, act):
        for u in range(2):
            b, axis, unit, k, half = chunk(i, u)
            for yes, tiles in places(unit, k, half):
                @pl.when(yes)
                def _():
                    for t, (which, row, col) in enumerate(tiles):
                        for n in range(3):
                            act(u, t, n, 7 * n + which, row, col)

    def fetch(i):
        slot = i % depth

        def get(u, t, n, which, row, col):
            pltpu.make_async_copy(tile(old[which], row, col), ins[n].at[slot, u, pl.ds(Q * t, Q), :], isem.at[n, slot, u]).start()

        moves(i, get)
        b, axis = chunk(i, 0)[:2]
        for n in range(3):
            @pl.when(axis == n)
            def _():
                for u in range(2):
                    pltpu.make_async_copy(r_refs[2 * n + u].at[b], g_s.at[slot, u], gsem.at[slot, u]).start()

    def real(i, then):
        for u in range(2):
            @pl.when(chunk(i, u)[2] < 31)
            def _():
                then(u)

    def stored(i):
        slot = i % depth

        def wait(u):
            for n in range(3):
                pltpu.make_async_copy(outs[n].at[slot, u], outs[n].at[slot, u], osem.at[n, slot, u]).wait()

        real(i, wait)

    def body(i):
        slot = i % depth

        @pl.when(i + depth - 1 < steps)
        def _():
            fetch(i + depth - 1)

        @pl.when(i >= depth)
        def _():
            stored(i - depth)

        for u in range(2):
            pltpu.make_async_copy(g_s.at[slot, u], g_s.at[slot, u], gsem.at[slot, u]).wait()

        def wait(u):
            for n in range(3):
                pltpu.make_async_copy(ins[n].at[slot, u], ins[n].at[slot, u], isem.at[n, slot, u]).wait()

        real(i, wait)

        def part(q):
            here = (slot, q // 4, pl.ds(pl.multiple_of(q % 4 * L, L), L))
            g = g_s[here].astype(F32)
            m = 0.9 * m_s[here] + 0.1 * g
            v = 0.95 * v_s[here] + 0.05 * g * g
            w = w_s[here].astype(F32)
            mo_s[here] = m
            vo_s[here] = v
            wo_s[here] = (w - 0.02 * (m * lax.rsqrt(v + 1e-8) + 0.1 * w)).astype(BF)

        loop(0, 8, part)

        def put(u, t, n, which, row, col):
            pltpu.make_async_copy(outs[n].at[slot, u, pl.ds(Q * t, Q), :], tile(new[which], row, col), osem.at[n, slot, u]).start()

        moves(i, put)

    for i in range(depth - 1):
        fetch(i)
    loop(0, steps, body)
    for i in range(depth):
        stored(steps - depth + i)


def adam(r, old, new, mine, depth=8):
    V, S = pltpu.VMEM, pltpu.SemaphoreType.DMA
    C = (depth, 2, RB // 2, L)
    given = [*r, *old, *new]
    return pl.pallas_call(
        functools.partial(_adam_kernel, mine=mine, depth=depth),
        in_specs=[ANY] * len(given),
        out_specs=[ANY] * len(old),
        out_shape=[jax.ShapeDtypeStruct(a.shape, a.dtype) for a in old],
        input_output_aliases={len(r) + len(old) + i: i for i in range(len(new))},
        scratch_shapes=[V(C, BF), V(C, BF), V(C, F32), V(C, F32), V(C, BF), V(C, F32), V(C, F32), S((depth, 2)), S((3, depth, 2)), S((3, depth, 2))],
        compiler_params=pltpu.CompilerParams(vmem_limit_bytes=ROOM),
        cost_estimate=pl.CostEstimate(flops=2 * 10**10, transcendentals=0, bytes_accessed=25 * 10**7),
    )(*given)


def swap(r, c):
    stride = STRIDES[c // 2]
    hop = lambda p: 3 - 2 * p if c % 2 else 1 - p % 2 * 2
    return lax.ppermute(r, "dp", [(dp, dp + hop(dp // stride % 4) * stride) for dp in range(64)])


def solution(mesh):
    angles = _angles()

    def step(x, dy, *arrays):
        arrays = [a[0] for a in arrays]
        wq, wk, wv, wo, wg, wu, wd = arrays[:7]
        x, dy = x[0], dy[0]
        cs = jnp.asarray(angles)
        q, k, v, at = qkv(x, cs, wq, wk, wv)
        o, ot, lse = attend(q, k, v)
        h, b, bt = out_norm(o, wo, x)
        _, r = backward(b, bt, dy, h, wg, wu, wd, ot, wo, q, k, v, lse, at, cs)
        others = [swap(r[c], c) for c in range(COLOURS)]
        new = adam(r, arrays, [], True)
        new = adam(others, arrays, new, False)
        return tuple(a[None] for a in new)

    states, all_of = P(("rep", "dp"), None, None), P(None, None, None)
    return jax.shard_map(step, mesh=mesh, in_specs=(states, states) + (all_of,) * 21, out_specs=(P("rep", None, None),) * 21, check_vma=False)
```

```python
import functools
import math

import jax
import jax.numpy as jnp
import numpy as np
from jax import lax
from jax.experimental import pallas as pl
from jax.experimental.pallas import tpu as pltpu
from jax.sharding import PartitionSpec as P

BF, F32 = jnp.bfloat16, jnp.float32
T, D, F, HEADS, KV, HEAD = 1024, 1280, 3072, 24, 2, 128
GROUP = HEADS // KV
THETA = 10000
NAMES = ("wq", "wk", "wv", "wo", "w_gate", "w_up", "w_down")
NEG = -1e30
HIDDEN = 2 * NEG
LOG2E = 1.4426950408889634
SCALE = HEAD**-0.5
ANY = pl.BlockSpec(memory_space=pl.ANY)
MESH = pl.DeviceIdType.MESH
Q, L, HALF = 256, 128, 64
ROWS = range(0, T, Q)
ROOM = 63 * 2**20

CHUNKS, BLOCKS, COLOURS = 156, 26, 6
RB = 1024
LATE = 22


def loop(first, last, body):
    lax.fori_loop(first, last, lambda i, _: body(i), None)


def _dot(a, b, ca=1, cb=0):
    return lax.dot_general(a, b, (((ca,), (cb,)), ((), ())), preferred_element_type=F32)


def _rms(wide):
    return lax.rsqrt(jnp.mean(wide**2, -1, keepdims=True) + 1e-6)


def _angles():
    half = HALF
    angle = np.arange(T, dtype=np.float32)[:, None] * (np.float32(THETA) ** (-np.arange(half, dtype=np.float32) / half)).astype(np.float32)
    angle = angle.astype(np.float64)
    return np.concatenate([np.cos(angle), np.sin(angle)], 1).astype(np.float32)


def _qkv_kernel(x_ref, cs_ref, wq_ref, wk_ref, wv_ref, q_ref, k_ref, v_ref, at_ref, a_s, c_s, s_s):
    i = pl.program_id(0)

    def norm(r):
        wide = x_ref[r : r + Q, :].astype(F32)
        a_s[r : r + Q, :] = (wide * _rms(wide)).astype(BF)
        cs = cs_ref[r : r + Q, :]
        sc = pltpu.roll(cs, HALF, 1)
        low = lax.broadcasted_iota(jnp.int32, cs.shape, 1) < HALF
        c_s[r : r + Q, :] = jnp.where(low, cs, sc)
        s_s[r : r + Q, :] = jnp.where(low, -sc, cs)

    def heads(r, w_ref, out_ref, turn):
        got = _dot(a_s[r : r + Q, :], w_ref[...])
        for n in range(w_ref.shape[1] // HEAD):
            t = got[:, n * HEAD : (n + 1) * HEAD].astype(BF)
            if turn:
                t = t.astype(F32)
                t = (t * c_s[r : r + Q, :] + pltpu.roll(t, HALF, 1) * s_s[r : r + Q, :]).astype(BF)
            out_ref[n, r : r + Q, :] = t

    @pl.when(i == 0)
    def _():
        for r in ROWS:
            norm(r)
            heads(r, wq_ref, q_ref, True)

    @pl.when((i > 0) & (i < 6))
    def _():
        at_ref[...] = a_s[:, pl.ds(pl.multiple_of((i - 1) * Q, Q), Q)].T
        for r in ROWS:
            heads(r, wq_ref, q_ref, True)

    @pl.when(i == 6)
    def _():
        for r in ROWS:
            heads(r, wk_ref, k_ref, True)
            heads(r, wv_ref, v_ref, False)


def qkv(x, cs, wq, wk, wv):
    whole = lambda *shape: pl.BlockSpec(shape, lambda i: (0,) * len(shape))
    last = lambda i: jnp.minimum(i, 5)
    return pl.pallas_call(
        _qkv_kernel,
        grid=(7,),
        in_specs=[whole(T, D), whole(T, HEAD), pl.BlockSpec((D, 4 * HEAD), lambda i: (0, last(i))), whole(D, Q), whole(D, Q)],
        out_specs=[pl.BlockSpec((4, T, HEAD), lambda i: (last(i), 0, 0)), whole(KV, T, HEAD), whole(KV, T, HEAD),
                   pl.BlockSpec((Q, T), lambda i: (jnp.clip(i - 1, 0, 4), 0))],
        out_shape=[jax.ShapeDtypeStruct((HEADS, T, HEAD), BF), jax.ShapeDtypeStruct((KV, T, HEAD), BF),
                   jax.ShapeDtypeStruct((KV, T, HEAD), BF), jax.ShapeDtypeStruct((D, T), BF)],
        scratch_shapes=[pltpu.VMEM((T, D), BF), pltpu.VMEM((T, HEAD), F32), pltpu.VMEM((T, HEAD), F32)],
        compiler_params=pltpu.CompilerParams(vmem_limit_bytes=ROOM),
    )(x, cs, wq, wk, wv)


def _attend_kernel(q_ref, k_ref, v_ref, o_ref, ot_ref, lse_ref, top_s, mix_s, *, bq, bk, wide):
    iq = pl.program_id(1)
    cols = GROUP * bq
    e = SCALE * LOG2E
    pieces = range(0, cols, wide)
    top_s[...] = jnp.full((1, cols), NEG, F32)
    mix_s[...] = jnp.zeros((HEAD + 8, cols), F32)
    ones = jnp.ones((8, bk), BF)

    def block(j, masked):
        here = pl.ds(pl.multiple_of(j * bk, bk), bk)
        scores = [_dot(k_ref[0, here, :], q_ref[...].reshape(cols, HEAD)[at : at + wide, :], 1, 1) for at in pieces]
        values = jnp.concatenate([v_ref[0, here, :].T, ones], axis=0)
        if masked:
            gap = lax.rem(lax.broadcasted_iota(jnp.int32, (bk, wide), 1), bq) - lax.broadcasted_iota(jnp.int32, (bk, wide), 0)
            ok = gap >= j * bk - iq * bq
        weights, keeps = [], []
        for at, s in zip(pieces, scores):
            if masked:
                s = jnp.where(ok, s, HIDDEN)
            old = top_s[:, at : at + wide]
            top = jnp.maximum(old, s.max(axis=0, keepdims=True))
            top_s[:, at : at + wide] = top
            weights.append(jnp.exp2((s - top) * e).astype(BF))
            keeps.append(jnp.exp2((old - top) * e))
        for at, p, keep in zip(pieces, weights, keeps):
            mix_s[:, at : at + wide] = mix_s[:, at : at + wide] * keep + _dot(values, p)

    loop(0, lax.div(iq * bq, bk), lambda j: block(j, False))
    loop(lax.div(iq * bq, bk), lax.div(iq * bq + bq + bk - 1, bk), lambda j: block(j, True))
    top, total = top_s[...], mix_s[HEAD : HEAD + 1, :]
    inverse = 1 / total
    lse = top * SCALE + jnp.log(total)
    for n in range(GROUP):
        out = (mix_s[:HEAD, n * bq : (n + 1) * bq] * inverse[:, n * bq : (n + 1) * bq]).astype(BF)
        ot_ref[n * HEAD : (n + 1) * HEAD, :] = out
        o_ref[:, n * HEAD : (n + 1) * HEAD] = out.T
        lse_ref[n] = lse[:, n * bq : (n + 1) * bq]


def attend(q, k, v, bq=Q, bk=Q, wide=2 * Q):
    return pl.pallas_call(
        functools.partial(_attend_kernel, bq=bq, bk=bk, wide=wide),
        grid=(KV, T // bq),
        in_specs=[pl.BlockSpec((GROUP, bq, HEAD), lambda h, i: (h, i, 0)), pl.BlockSpec((1, T, HEAD), lambda h, i: (h, 0, 0)),
                  pl.BlockSpec((1, T, HEAD), lambda h, i: (h, 0, 0))],
        out_specs=[pl.BlockSpec((bq, GROUP * HEAD), lambda h, i: (i, h)), pl.BlockSpec((GROUP * HEAD, bq), lambda h, i: (h, i)),
                   pl.BlockSpec((GROUP, 1, bq), lambda h, i: (h, 0, i))],
        out_shape=[jax.ShapeDtypeStruct((T, HEADS * HEAD), BF), jax.ShapeDtypeStruct((HEADS * HEAD, T), BF),
                   jax.ShapeDtypeStruct((HEADS, 1, T), F32)],
        scratch_shapes=[pltpu.VMEM((1, GROUP * bq), F32), pltpu.VMEM((HEAD + 8, GROUP * bq), F32)],
        compiler_params=pltpu.CompilerParams(vmem_limit_bytes=ROOM),
            )(q, k, v)


def _out_kernel(o_ref, wo_ref, x_ref, h_ref, b_ref, bt_ref):
    h = (x_ref[...].astype(F32) + _dot(o_ref[...], wo_ref[...]).astype(BF).astype(F32)).astype(BF)
    h_ref[...] = h
    wide = h.astype(F32)
    b = (wide * _rms(wide)).astype(BF)
    b_ref[...] = b
    bt_ref[...] = b.T


def out_norm(o, wo, x, rows=Q):
    spec = lambda width: pl.BlockSpec((rows, width), lambda i: (i, 0))
    return pl.pallas_call(
        _out_kernel,
        grid=(T // rows,),
        in_specs=[spec(HEADS * HEAD), pl.BlockSpec((HEADS * HEAD, D), lambda i: (0, 0)), spec(D)],
        out_specs=[spec(D), spec(D), pl.BlockSpec((D, rows), lambda i: (0, i))],
        out_shape=[jax.ShapeDtypeStruct((T, D), BF), jax.ShapeDtypeStruct((T, D), BF), jax.ShapeDtypeStruct((D, T), BF)],
        compiler_params=pltpu.CompilerParams(vmem_limit_bytes=ROOM),
        cost_estimate=pl.CostEstimate(flops=2 * T * D * 3072, transcendentals=0, bytes_accessed=10**7),
    )(o, wo, x)


STRIDES = (16, 4, 1)


def near_bit(place):
    return (place + 1) // 2 % 2


def rows(at, n):
    return pl.ds(pl.multiple_of(at, 16), n)


def block_at(place):
    return (place >= 0) & (place < BLOCKS + 1) & (place != LATE), place - (place + 31 - LATE) // 32


class Comm:
    STEPS, SLOTS, LINE, PIECE = 9, 4, RB >> 4, RB >> 6
    END = BLOCKS + 1 + 2 * STEPS

    @staticmethod
    def scratch():
        V, S, n = pltpu.VMEM, pltpu.SemaphoreType.DMA, Comm.SLOTS
        return [V((COLOURS, n, RB, L), BF), V((COLOURS, n, RB // 2 + Comm.LINE, L), BF), V((COLOURS, 2, RB // 2, L), F32),
                V((COLOURS, n, RB // 2, L), BF), S((Comm.STEPS + 4, COLOURS, n)), S((Comm.STEPS + 4, COLOURS, n)), S((COLOURS, n)), S((COLOURS, n))]

    def __init__(self, g, r, refs):
        self.g, self.r = g, r
        self.recv, self.send, self.acc, self.loc, self.ssem, self.rsem, self.lsem, self.osem = refs
        dp = lax.axis_index("dp")
        self.place = [dp // n % 4 for n in STRIDES]
        self.bits = [[near_bit(c) for c in self.place], [c // 2 for c in self.place]]
        self.others = [[c + 1 - c % 2 * 2 for c in self.place], [3 - c for c in self.place], [(c + 2) % 4 for c in self.place]]
        self.nexts = [[dp + (o - c) * n for o, c, n in zip(other, self.place, STRIDES)] for other in self.others]

    def barrier(self):
        sem = pltpu.get_barrier_semaphore()
        for nexts in self.nexts:
            for n in nexts:
                pl.semaphore_signal(sem, device_id={"dp": n}, device_id_type=MESH)
        pl.semaphore_wait(sem, 9)

    def last(self, c):
        return (c // 2 + 2) % 3

    def bit(self, c, k):
        return self.bits[(k ^ c) % 2][(c // 2 + k // 2) % 3]

    def row(self, c, k):
        at = 0
        for i in range(1, k):
            at = at + self.bit(c, i) * (RB >> (i + 1))
        return at

    def half(self, c, b, bit):
        return self.g.at[COLOURS * b + c, rows(bit * (RB // 2), RB // 2), :]

    def mine(self, c, b, k):
        return self.r[c].at[b, rows(self.row(c, k), RB >> k), :]

    def piece(self, c, b):
        n = self.PIECE
        return self.r[c].at[b, rows(self.row(c, 4) + self.place[self.last(c)] * n, n), :]

    def finished(self, c, p):
        return self.send.at[c, p, pl.ds(RB // 2, self.PIECE), :]

    def copies(self, s, c, b, p):
        def copy(src, dst, device, number):
            return pltpu.make_async_remote_copy(src_ref=src, dst_ref=dst, send_sem=self.ssem.at[number, c, p], recv_sem=self.rsem.at[number, c, p],
                                                device_id={"dp": device}, device_id_type=MESH)

        if s in (4, 5):
            axis, n = self.last(c), self.PIECE
            out = []
            for i in range(3):
                if s == 4:
                    src = self.send.at[c, p, rows(RB // 2 - self.LINE + self.others[i][axis] * n, n), :]
                    dst = self.recv.at[c, p, pl.ds(RB - self.LINE + i * n, n), :]
                else:
                    src, dst = self.finished(c, p), self.piece(c, b)
                out.append(copy(src, dst, self.nexts[i][axis], 3 * s - 8 + i))
            return out
        k = s if s < 4 else self.STEPS - s
        n = RB >> (k + 1)
        if s < 4:
            src = self.half(c, b, 1 - self.bit(c, 0)) if s == 0 else self.send.at[c, p, pl.ds(RB // 2 - 2 * n, n), :]
            dst = self.recv.at[c, p, pl.ds(RB - 2 * n, n), :]
        else:
            src = dst = self.mine(c, b, k + 1)
        return [copy(src, dst, self.nexts[(k ^ c) % 2][(c // 2 + k // 2) % 3], s if s < 4 else s + 4)]

    def local(self, c, b, p):
        return pltpu.make_async_copy(self.half(c, b, self.bit(c, 0)), self.loc.at[c, p], self.lsem.at[c, p])

    def own(self, c, b, p):
        return pltpu.make_async_copy(self.finished(c, p), self.piece(c, b), self.osem.at[c, p])

    def step(self, s, b):
        p, pa = b % self.SLOTS, b % 2
        for c in range(COLOURS):
            if s:
                for d in self.copies(s - 1, c, b, p):
                    d.wait_recv()
            if s == 0:
                self.local(c, b, p).start()
            elif s <= 4:
                n = RB >> s
                h = n // 2 if s < 4 else n
                if s == 1:
                    self.local(c, b, p).wait()

                def total(at):
                    came = self.recv[c, p, rows(RB - 2 * n + at, h), :].astype(F32)
                    if s == 1:
                        return self.loc[c, p, rows(at, h), :].astype(F32) + came
                    return self.acc[c, pa, rows(RB // 2 - 2 * n + at, h), :] + came

                if s < 4:
                    self.send[c, p, RB // 2 - n : RB // 2 - n + h, :] = total((1 - self.bit(c, s)) * h).astype(BF)
                else:
                    every = total(0)
                    self.acc[c, pa, RB // 2 - n :, :] = every
                    self.send[c, p, RB // 2 - n : RB // 2, :] = every.astype(BF)
            elif s == 5:
                n = self.PIECE
                done = self.acc[c, pa, rows(RB // 2 - self.LINE + self.place[self.last(c)] * n, n), :]
                for i in range(3):
                    done = done + self.recv[c, p, RB - self.LINE + i * n : RB - self.LINE + (i + 1) * n, :].astype(F32)
                self.send[c, p, RB // 2 : RB // 2 + n, :] = done.astype(BF)
                self.own(c, b, p).start()
            elif s == 6:
                self.own(c, b, p).wait()
            if s < self.STEPS:
                for d in self.copies(s, c, b, p):
                    d.start()
            if 0 < s < 4:
                self.acc[c, pa, RB // 2 - n : RB // 2 - n + h, :] = total(self.bit(c, s) * h)

    def tick(self, t):
        for s in range(self.STEPS, -1, -1):
            valid, b = block_at(t - 2 * s)

            @pl.when(valid)
            def _():
                self.step(s, b)

            if s < self.STEPS:
                valid1, b1 = block_at(t - 2 * s - 2)

                @pl.when(valid1)
                def _():
                    for c in range(COLOURS):
                        for d in self.copies(s, c, b1, b1 % self.SLOTS):
                            d.wait_send()

    def ticks(self, first, last):
        loop(first, last, self.tick)


def _put(stage, value, k):
    stage[k, :Q, :] = value[:, :L].astype(BF)
    stage[k, Q:, :] = value[:, L:].astype(BF)


def _backward_kernel(b_ref, bt_ref, dy_ref, h_ref, wg_ref, wu_ref, wd_ref, ot_ref, wo_ref, q_ref, k_ref, v_ref, lse_ref, at_ref, cs_ref,
                     g_ref, *rest):
    r_refs, rest = rest[:6], rest[6:]
    stage, dh_s, dot_s, delta_s, isem, wsem, osem, *refs = rest
    comm = Comm(g_ref, r_refs, refs)
    comm.barrier()
    ticks = comm.ticks

    def load(src, dst, n):
        return pltpu.make_async_copy(src, dst, isem.at[n])

    def out(slot, unit, half):
        return pltpu.make_async_copy(stage.at[slot], g_ref.at[pl.ds(unit * 5, 5), pl.ds(half * 512, 512), :], osem.at[slot])

    def mlp(b_s, bt_s, dy_s, db_s, wg_s, wu_s, wd_s, act_s, dg_s, du_s):
        firsts = [load(b_ref, b_s, 0), load(bt_ref, bt_s, 1), load(dy_ref, dy_s, 2)]
        for d in firsts:
            d.start()

        def weights(j, slot):
            here = pl.ds(pl.multiple_of(j * Q, Q), Q)
            return [pltpu.make_async_copy(src, dst.at[slot], wsem.at[slot, n]) for n, (src, dst) in enumerate(
                ((wg_ref.at[:, here], wg_s), (wu_ref.at[:, here], wu_s), (wd_ref.at[here, :], wd_s)))]

        for d in weights(0, 0):
            d.start()
        db_s[...] = jnp.zeros_like(db_s)
        for d in firsts:
            d.wait()

        def outs(j):
            return [out(n, 3 * (j // 2) + n, j % 2) for n in range(3)]

        def upto_j(j):
            return jnp.maximum(j - 1, 0)

        def body(j):
            slot = j % 2

            @pl.when(j < 11)
            def _():
                for d in weights(j + 1, 1 - slot):
                    d.start()

            for d in weights(j, slot):
                d.wait()
            for r in ROWS:
                gate = _dot(b_s[r : r + Q, :], wg_s[slot])
                up = _dot(b_s[r : r + Q, :], wu_s[slot])
                da = _dot(dy_s[r : r + Q, :], wd_s[slot], 1, 1).astype(BF).astype(F32)
                sig = 1 / (1 + jnp.exp(-gate))
                silu = gate * sig
                act_s[:, r : r + Q] = (silu * up).astype(BF).T
                du_s[r : r + Q, :] = (da * silu).astype(BF)
                dg_s[r : r + Q, :] = (da * up * (sig + silu * (1 - sig))).astype(BF)

            @pl.when(j > 0)
            def _():
                for d in outs(j - 1):
                    d.wait()

            ticks(upto_j(j - 1), upto_j(j))
            for k in range(5):
                _put(stage.at[0], _dot(act_s[...], dy_s[:, k * Q : (k + 1) * Q]), k)
                _put(stage.at[1], _dot(bt_s[k * Q : (k + 1) * Q, :], dg_s[...]), k)
                _put(stage.at[2], _dot(bt_s[k * Q : (k + 1) * Q, :], du_s[...]), k)
            for d in outs(j):
                d.start()
            for r in ROWS:
                db_s[r : r + Q, :] += _dot(dg_s[r : r + Q, :], wg_s[slot], 1, 1) + _dot(du_s[r : r + Q, :], wu_s[slot], 1, 1)

        loop(0, 12, body)
        for d in outs(11):
            d.wait()
        load(h_ref, b_s, 0).start()
        load(h_ref, b_s, 0).wait()
        for r in range(0, T, L):
            wide = b_s[r : r + L, :].astype(F32)
            scale = _rms(wide)
            db = db_s[r : r + L, :].astype(BF).astype(F32)
            back = db * scale - wide * (scale**3 * jnp.mean(db * wide, -1, keepdims=True))
            dh_s[r : r + L, :] = (dy_s[r : r + L, :].astype(F32) + back.astype(BF).astype(F32)).astype(BF)

    V = pltpu.VMEM
    pl.run_scoped(mlp, V((T, D), BF), V((D, T), BF), V((T, D), BF), V((T, D), F32), V((2, D, Q), BF), V((2, D, Q), BF), V((2, Q, D), BF),
                  V((Q, T), BF), V((T, Q), BF), V((T, Q), BF))

    def rest_of_layer(ot_s, wo_s, q_s, dq_s, at_s, k_s, kt_s, v_s, lse_s, cs_s, cst_s, dqt_s, dk_s, dv_s):
        firsts = [load(s, d, n) for n, (s, d) in enumerate(
            ((q_ref, q_s), (at_ref, at_s), (k_ref, k_s), (v_ref, v_s), (lse_ref, lse_s), (cs_ref, cs_s)))]

        def parts(i, slot):
            here = pl.ds(pl.multiple_of(i * Q, Q), Q)
            return [pltpu.make_async_copy(ot_ref.at[here, :], ot_s.at[slot], wsem.at[slot, 0]),
                    pltpu.make_async_copy(wo_ref.at[here, :], wo_s.at[slot], wsem.at[slot, 1])]

        for d in parts(0, 0) + firsts:
            d.start()

        def outs(i):
            return out(i % 2, 18 + (i // 2), i % 2)

        def project(i):
            slot = i % 2

            @pl.when(i < 11)
            def _():
                for d in parts(i + 1, 1 - slot):
                    d.start()

            for d in parts(i, slot):
                d.wait()
            here = pl.ds(pl.multiple_of(i * Q, Q), Q)
            do = _dot(wo_s[slot], dh_s[...], 1, 1).astype(BF)
            dot_s[here, :] = do
            both = do.astype(F32) * ot_s[slot].astype(F32)
            for n in range(2):
                delta_s[2 * i + n] = both[n * L : (n + 1) * L, :].sum(0, keepdims=True)
            for k in range(5):
                _put(stage.at[slot], _dot(ot_s[slot], dh_s[:, k * Q : (k + 1) * Q]), k)
            outs(i).start()

            @pl.when(i > 0)
            def _():
                outs(i - 1).wait()

        e = SCALE * LOG2E
        bq, bk, wide = L, Q, 512
        cols = GROUP * bq

        def turned_back(t, here):
            t = t.astype(BF).astype(F32)
            cos, sin = cst_s[:HALF, here], cst_s[HALF:, here]
            a, b = t[:HALF, :], t[HALF:, :]
            return jnp.concatenate([a * cos + b * sin, b * cos - a * sin], 0).astype(BF)

        def attention(n):
            ih, iq = (n // 8), n % 8
            at = pl.ds(pl.multiple_of(iq * bq, bq), bq)
            heads = ih * GROUP

            @pl.when(iq == 0)
            def _():
                dk_s[...] = jnp.zeros_like(dk_s)
                dv_s[...] = jnp.zeros_like(dv_s)

            dqt_s[...] = jnp.zeros_like(dqt_s)

            def row(ref):
                return jnp.concatenate([ref[heads + m, :, at] for m in range(GROUP)], axis=1)

            lses, deltas = row(lse_s) * LOG2E, row(delta_s)

            def block(j, masked):
                here = pl.ds(pl.multiple_of(j * bk, bk), bk)
                kj, vj, ktj = k_s[ih, here, :], v_s[ih, here, :], kt_s[ih, :, here]
                if masked:
                    gap = lax.rem(lax.broadcasted_iota(jnp.int32, (bk, wide), 1), bq) - lax.broadcasted_iota(jnp.int32, (bk, wide), 0)
                    ok = gap >= j * bk - iq * bq
                per = wide // bq
                qs = [q_s[pl.ds(heads + m, per), at, :].reshape(wide, HEAD) for m in range(0, GROUP, per)]
                dos = [jnp.concatenate([dot_s[pl.ds(pl.multiple_of((heads + m + i) * HEAD, HEAD), HEAD), at] for i in range(per)], axis=1)
                       for m in range(0, GROUP, per)]
                scores = [_dot(kj, x, 1, 1) for x in qs]
                dps = [_dot(vj, x) for x in dos]
                for m in range(cols // wide):
                    span = slice(m * wide, (m + 1) * wide)
                    p = jnp.exp2(scores[m] * e - lses[:, span])
                    if masked:
                        p = jnp.where(ok, p, 0.0)
                    ds = (p * (dps[m] - deltas[:, span])).astype(BF)
                    dv_s[here, :] += _dot(p.astype(BF), dos[m], 1, 1)
                    dk_s[here, :] += _dot(ds, qs[m])
                    dqt_s[:, span] += _dot(ktj, ds)

            loop(0, iq // 2, lambda j: block(j, False))
            block(iq // 2, True)
            for m in range(GROUP):
                dq_s[m * HEAD : (m + 1) * HEAD, at] = turned_back(dqt_s[:, m * bq : (m + 1) * bq] * SCALE, at)

            @pl.when(iq == 7)
            def _():
                def product(i, part):
                    slot = i % 2

                    @pl.when(i > 1)
                    def _():
                        out(slot, 0, 0).wait()

                    for k in range(5):
                        _put(stage.at[slot], _dot(at_s[k * Q : (k + 1) * Q, :], part, 1, 1), k)

                def one(i):
                    product(i, dq_s[pl.ds(pl.multiple_of(i * Q, Q), Q), :])
                    out(i % 2, 24 + 3 * ih + (i // 2), i % 2).start()

                loop(0, 6, one)
                dk = turned_back((dk_s[...] * SCALE).T, pl.ds(0, T))
                product(6, jnp.concatenate([dk, dv_s[...].T.astype(BF)], 0))
                out(0, 30, ih).start()
                out(1, 0, 0).wait()
                out(0, 0, 0).wait()

        def done(n):
            return jnp.where(n < 12, 10 + (n + 1) // 3, jnp.where(n < 28, 14 + (n - 11) * 5 // 8, Comm.END))

        def body(n):
            @pl.when(n < 12)
            def _():
                project(n)

            @pl.when(n == 12)
            def _():
                outs(11).wait()
                for d in firsts:
                    d.wait()
                for i in range(KV):
                    kt_s[i] = k_s[i].T
                cst_s[...] = cs_s[...].T

            @pl.when((n >= 12) & (n < 28))
            def _():
                attention(n - 12)

            ticks(done(n - 1), done(n))

        loop(0, 29, body)

    pl.run_scoped(rest_of_layer, V((2, Q, T), BF), V((2, Q, D), BF), V((HEADS, T, HEAD), BF), V((GROUP * HEAD, T), BF), V((D, T), BF),
                  V((KV, T, HEAD), BF), V((KV, HEAD, T), BF), V((KV, T, HEAD), BF), V((HEADS, 1, T), F32), V((T, HEAD), F32), V((HEAD, T), F32),
                  V((HEAD, GROUP * L), F32), V((T, HEAD), F32), V((T, HEAD), F32))


def backward(b, bt, dy, h, wg, wu, wd, ot, wo, q, k, v, lse, at, cs):
    V, S = pltpu.VMEM, pltpu.SemaphoreType.DMA
    outs = pl.pallas_call(
        _backward_kernel,
        in_specs=[ANY] * 15,
        out_specs=[ANY] * 7,
        out_shape=[jax.ShapeDtypeStruct((CHUNKS, RB, L), BF)] + [jax.ShapeDtypeStruct((BLOCKS, RB // 2, L), BF)] * 6,
        scratch_shapes=[V((3, 5, 512, L), BF), V((T, D), BF), V((HEADS * HEAD, T), BF), V((HEADS, 1, T), F32), S((6,)), S((2, 3)), S((3,)),
                        *Comm.scratch()],
        compiler_params=pltpu.CompilerParams(collective_id=0, has_side_effects=True, vmem_limit_bytes=ROOM),
    )(b, bt, dy, h, wg, wu, wd, ot, wo, q, k, v, lse, at, cs)
    return outs[0], outs[1:]


def _adam_kernel(*refs, mine, depth):
    r_refs, old, new = refs[:6], refs[6:27], refs[-31:-10]
    g_s, w_s, m_s, v_s, wo_s, mo_s, vo_s, gsem, isem, osem = refs[-10:]
    dp = lax.axis_index("dp")
    ins, outs = (w_s, m_s, v_s), (wo_s, mo_s, vo_s)
    number = {name: i for i, name in enumerate(NAMES)}
    steps = CHUNKS // 2

    def chunk(i, u):
        axis = i % 3
        place = jnp.where(axis == 0, dp // STRIDES[0], jnp.where(axis == 1, dp // STRIDES[1] % 4, dp % 4))
        bit = place // 2 if u else near_bit(place)
        at = 2 * i + u
        return i // 3, axis, at // 5, at % 5, bit if mine else 1 - bit

    def places(unit, k, half):
        tall = lambda name, n: [(number[name], 512 * n + Q * half, Q * k + L * t) for t in range(2)]
        flat = lambda name, n: [(number[name], Q * k, 512 * n + Q * half + L * t) for t in range(2)]
        third = unit % 3
        return [((unit < 18) & (third == 0), tall("w_down", unit // 3)), ((unit < 18) & (third == 1), flat("w_gate", unit // 3)),
                ((unit < 18) & (third == 2), flat("w_up", unit // 3)), ((unit >= 18) & (unit < 24), tall("wo", unit - 18)),
                ((unit >= 24) & (unit < 30), flat("wq", unit - 24)),
                (unit == 30, [(number[name], Q * k, L * half) for name in ("wk", "wv")])]

    def tile(ref, row, col):
        return ref.at[pl.ds(pl.multiple_of(row, Q), Q), pl.ds(pl.multiple_of(col, L), L)]

    def moves(i, act):
        for u in range(2):
            b, axis, unit, k, half = chunk(i, u)
            for yes, tiles in places(unit, k, half):
                @pl.when(yes)
                def _():
                    for t, (which, row, col) in enumerate(tiles):
                        for n in range(3):
                            act(u, t, n, 7 * n + which, row, col)

    def fetch(i):
        slot = i % depth

        def get(u, t, n, which, row, col):
            pltpu.make_async_copy(tile(old[which], row, col), ins[n].at[slot, u, pl.ds(Q * t, Q), :], isem.at[n, slot, u]).start()

        moves(i, get)
        b, axis = chunk(i, 0)[:2]
        for n in range(3):
            @pl.when(axis == n)
            def _():
                for u in range(2):
                    pltpu.make_async_copy(r_refs[2 * n + u].at[b], g_s.at[slot, u], gsem.at[slot, u]).start()

    def real(i, then):
        for u in range(2):
            @pl.when(chunk(i, u)[2] < 31)
            def _():
                then(u)

    def stored(i):
        slot = i % depth

        def wait(u):
            for n in range(3):
                pltpu.make_async_copy(outs[n].at[slot, u], outs[n].at[slot, u], osem.at[n, slot, u]).wait()

        real(i, wait)

    def body(i):
        slot = i % depth

        @pl.when(i + depth - 1 < steps)
        def _():
            fetch(i + depth - 1)

        @pl.when(i >= depth)
        def _():
            stored(i - depth)

        for u in range(2):
            pltpu.make_async_copy(g_s.at[slot, u], g_s.at[slot, u], gsem.at[slot, u]).wait()

        def wait(u):
            for n in range(3):
                pltpu.make_async_copy(ins[n].at[slot, u], ins[n].at[slot, u], isem.at[n, slot, u]).wait()

        real(i, wait)

        def part(q):
            here = (slot, q // 4, pl.ds(pl.multiple_of(q % 4 * L, L), L))
            g = g_s[here].astype(F32)
            m = 0.9 * m_s[here] + 0.1 * g
            v = 0.95 * v_s[here] + 0.05 * g * g
            w = w_s[here].astype(F32)
            mo_s[here] = m
            vo_s[here] = v
            wo_s[here] = (w - 0.02 * (m * lax.rsqrt(v + 1e-8) + 0.1 * w)).astype(BF)

        loop(0, 8, part)

        def put(u, t, n, which, row, col):
            pltpu.make_async_copy(outs[n].at[slot, u, pl.ds(Q * t, Q), :], tile(new[which], row, col), osem.at[n, slot, u]).start()

        moves(i, put)

    for i in range(depth - 1):
        fetch(i)
    loop(0, steps, body)
    for i in range(depth):
        stored(steps - depth + i)


def adam(r, old, new, mine, depth=8):
    V, S = pltpu.VMEM, pltpu.SemaphoreType.DMA
    C = (depth, 2, RB // 2, L)
    given = [*r, *old, *new]
    return pl.pallas_call(
        functools.partial(_adam_kernel, mine=mine, depth=depth),
        in_specs=[ANY] * len(given),
        out_specs=[ANY] * len(old),
        out_shape=[jax.ShapeDtypeStruct(a.shape, a.dtype) for a in old],
        input_output_aliases={len(r) + len(old) + i: i for i in range(len(new))},
        scratch_shapes=[V(C, BF), V(C, BF), V(C, F32), V(C, F32), V(C, BF), V(C, F32), V(C, F32), S((depth, 2)), S((3, depth, 2)), S((3, depth, 2))],
        compiler_params=pltpu.CompilerParams(vmem_limit_bytes=ROOM),
        cost_estimate=pl.CostEstimate(flops=2 * 10**10, transcendentals=0, bytes_accessed=25 * 10**7),
    )(*given)


def swap(r, c):
    stride = STRIDES[c // 2]
    hop = lambda p: 3 - 2 * p if c % 2 else 1 - p % 2 * 2
    return lax.ppermute(r, "dp", [(dp, dp + hop(dp // stride % 4) * stride) for dp in range(64)])


def solution(mesh):
    angles = _angles()

    def step(x, dy, *arrays):
        arrays = [a[0] for a in arrays]
        wq, wk, wv, wo, wg, wu, wd = arrays[:7]
        x, dy = x[0], dy[0]
        cs = jnp.asarray(angles)
        q, k, v, at = qkv(x, cs, wq, wk, wv)
        o, ot, lse = attend(q, k, v)
        h, b, bt = out_norm(o, wo, x)
        _, r = backward(b, bt, dy, h, wg, wu, wd, ot, wo, q, k, v, lse, at, cs)
        others = [swap(r[c], c) for c in range(COLOURS)]
        new = adam(r, arrays, [], True)
        new = adam(others, arrays, new, False)
        return tuple(a[None] for a in new)

    states, all_of = P(("rep", "dp"), None, None), P(None, None, None)
    return jax.shard_map(step, mesh=mesh, in_specs=(states, states) + (all_of,) * 21, out_specs=(P("rep", None, None),) * 21, check_vma=False)
```
